32 devices in a mesh: pipe: 4 (over z), dp: 4 (over x, core), expert: 2 (over y).
Axes of the slice: x: 2, y: 2, z: 4, core: 2. Of those that a mesh axis runs over, the one named last changes fastest.
Arguments:
- entering: bfloat16 [4, 512, 4096], P('pipe', 'dp', 'expert'), may hold values from -6 to 6
- pending: bfloat16 [4, 512, 4096], P('pipe', 'dp', 'expert'), may hold values from -6 to 6
- stashed_in: bfloat16 [4, 512, 4096], P('pipe', 'dp', 'expert'), may hold values from -6 to 6
- forward_routes: int32 [4, 512, 2], P('pipe', 'dp'), may hold values from 0 to 3, all different within a row; in each aligned block of 128 rows (0 to 127, 128 to 255, ..., all dimensions but the last counted through in order) at most 64 rows name the same one
- backward_routes: int32 [4, 512, 2], P('pipe', 'dp'), may hold values from 0 to 3, all different within a row; in each aligned block of 128 rows (0 to 127, 128 to 255, ..., all dimensions but the last counted through in order) at most 64 rows name the same one
- norm_gains: float32 [4, 4096], P('pipe', 'expert'), may hold values from 0.5 to 1.5
- w_router: bfloat16 [4, 4096, 4], P('pipe', 'expert'), may hold values from -0.09375 to 0.09375
- w_gateup: bfloat16 [4, 4, 4096, 2, 1024], P('pipe', 'dp', None, None, 'expert'), may hold values from -0.09375 to 0.09375
- w_down: bfloat16 [4, 4, 1024, 4096], P('pipe', 'dp', 'expert'), may hold values from -0.1875 to 0.1875
Outputs:
- forward_out: bfloat16 [4, 512, 4096], P('pipe', 'dp', 'expert')
- input_grads: bfloat16 [4, 512, 4096], P('pipe', 'dp', 'expert')
- passed_forward: bfloat16 [4, 512, 4096], P('pipe', 'dp', 'expert')
- passed_backward: bfloat16 [4, 512, 4096], P('pipe', 'dp', 'expert')
- gain_grads: float32 [4, 4096], P('pipe', 'expert')
The draws below stay inside these ranges and needn't reach their ends.
Inputs may be any that keep to these rules, and one draw needn't show every extreme that they name: `forward_routes`: each row names 2 different experts; in each aligned block of 128 rows (one sequence) every expert is named by exactly 64 rows. `backward_routes`: each row names 2 different experts; in each aligned block of 128 rows (one sequence) every expert is named by exactly 64 rows.
All inputs are finite; a program needn't handle non-finite values.
Results may differ from the reference program's by a relative error of at most 0.015.
Values may be sent and summed in bfloat16 or wider, within the bound.
A program may use at most 64 MiB of HBM per device.

```python
import math
import jax
import jax.numpy as jnp
import numpy as np
from jax import lax

D = 4096
FF = 1024
TOPK = 2
TOK = 128
EXPERTS = 4
TOKENS = 512
CAP = 64
N_PIPE = 4
N_EXPERT = 2


def shard_levels(stream_key, dims, split, least, high):
    factor_of, own = 1.0, jax.random.fold_in(stream_key, 6)
    for dim, shards_of in split:
        heights = jnp.exp(jax.random.uniform(jax.random.fold_in(own, dim), (shards_of,), jnp.float32, least / len(split), high / len(split)))
        factor_of = factor_of * jnp.repeat(heights, dims[dim] // shards_of).reshape([-1 if axis == dim else 1 for axis in range(len(dims))])
    return factor_of


def shared_out(stream_key, own, number, rows, count, top, most, skew):
    order = jax.random.permutation(stream_key, count)
    packed, ordinary = portions_of(count, rows * top, most, skew, True), portions_of(count, rows * top, most, skew, False)
    places = jnp.arange(count)

    def named(lengths, offset_by):
        used = int((lengths > 0).sum())
        fixed = max(1, used // 4)
        shifted = fixed + (places - fixed + offset_by * (used - fixed)) % max(1, count - fixed)
        return jnp.zeros((count,), jnp.int32).at[order[jnp.where(places < fixed, places, shifted)]].set(jnp.asarray(lengths, jnp.int32))

    lengths = jnp.where(number % 4 == 0, named(packed, number // 4), named(ordinary, number - number // 4 - 1))
    mixed = jax.random.permutation(jax.random.fold_in(own, 3), count)
    source_of, receiver = mixed[0:count // 2 * 2:2], mixed[1:count // 2 * 2:2]
    room = jnp.minimum(lengths[source_of] - 1, most - lengths[receiver]) // 2
    room = jnp.where((source_of == order[0]) | (receiver == order[0]) | (lengths[receiver] == 0), 0, jnp.maximum(room, 0))
    shifted = jax.random.randint(jax.random.fold_in(own, 4), (count // 2,), 0, 1 << 20) % (room + 1)
    lengths = lengths.at[source_of].add(-shifted).at[receiver].add(shifted)
    items = jnp.searchsorted(jnp.cumsum(lengths), jnp.arange(rows * top), side="right").astype(jnp.int32)
    listing = items.reshape(top, rows).T
    listing = listing[jax.random.permutation(jax.random.fold_in(own, 1), rows)]
    offset_by = jax.random.randint(jax.random.fold_in(own, 2), (rows, 1), 0, top)
    return jnp.take_along_axis(listing, (jnp.arange(top)[None, :] + offset_by) % top, axis=1)


def portions_of(amount, total, limit, slope, full):
    portions = [(1 << 20) // math.isqrt(grade ** slope) + 1 for grade in range(1, amount + 1)]
    largest = limit if full else min(limit, max(-(-total // amount), total * portions[0] // sum(portions)))
    least = 1 if total - largest >= amount - 1 else 0
    holding, spare = [largest] + [least] * (amount - 1), total - largest - least * (amount - 1)
    while spare > 0:
        movable = [i for i in range(1, amount) if holding[i] < largest] or [i for i in range(1, amount) if holding[i] < limit]
        whole, remaining = sum([portions[i] for i in movable]), spare
        for i in movable:
            extra = min(limit - holding[i], max(1, remaining * portions[i] // whole), spare)
            holding[i] = holding[i] + extra
            spare = spare - extra
    return np.array(holding)


def noise(key, shape, spread, bound, cuts=(), held_as=jnp.bfloat16):
    values = spread * jax.random.normal(key, shape, jnp.float32)
    if cuts:
        values = values * shard_levels(key, shape, cuts, -0.22, 0.18)
    return jnp.clip(values, -bound, bound).astype(held_as)


def setup_inputs(seed: int = 0) -> dict:
    key_of = jax.random.split(jax.random.key(seed), 10)
    entering = noise(key_of[0], (N_PIPE, TOKENS, D), 1.0, 6.0, ((0, 4), (1, 4), (2, 2)))
    pending = noise(key_of[1], (N_PIPE, TOKENS, D), 1.0, 6.0, ((0, 4), (1, 4), (2, 2)))
    stashed_in = noise(key_of[2], (N_PIPE, TOKENS, D), 1.0, 6.0, ((0, 4), (1, 4), (2, 2)))
    forward_routes_keys = jax.random.split(jax.random.fold_in(key_of[3], 1), N_PIPE * TOKENS // TOK)
    forward_routes_turns = jax.random.permutation(jax.random.fold_in(key_of[3], 3), N_PIPE * TOKENS // TOK)
    forward_routes = jax.vmap(lambda own, number: shared_out(jax.random.fold_in(key_of[3], 2), own, number, TOK, EXPERTS, TOPK, CAP, 0))(forward_routes_keys, forward_routes_turns).reshape((N_PIPE, TOKENS, TOPK))
    backward_routes_keys = jax.random.split(jax.random.fold_in(key_of[4], 1), N_PIPE * TOKENS // TOK)
    backward_routes_turns = jax.random.permutation(jax.random.fold_in(key_of[4], 3), N_PIPE * TOKENS // TOK)
    backward_routes = jax.vmap(lambda own, number: shared_out(jax.random.fold_in(key_of[4], 2), own, number, TOK, EXPERTS, TOPK, CAP, 0))(backward_routes_keys, backward_routes_turns).reshape((N_PIPE, TOKENS, TOPK))
    norm_gains = jnp.clip(1.0 + 0.1 * jax.random.normal(key_of[5], (N_PIPE, D), jnp.float32), 0.5, 1.5)
    w_router = noise(key_of[6], (N_PIPE, D, EXPERTS), D ** -0.5, 0.09375, ((0, 4), (1, 2)))
    w_gateup = noise(key_of[7], (N_PIPE, EXPERTS, D, 2, FF), D ** -0.5, 0.09375, ((0, 4), (1, 4), (4, 2)))
    w_down = noise(key_of[8], (N_PIPE, EXPERTS, FF, D), FF ** -0.5, 0.1875, ((0, 4), (1, 4), (2, 2)))
    return dict(entering=entering, pending=pending, stashed_in=stashed_in, forward_routes=forward_routes, backward_routes=backward_routes, norm_gains=norm_gains, w_router=w_router, w_gateup=w_gateup, w_down=w_down)


ROUTE_SCALE = 2.827
EPSILON = 1e-05

def slot_places(routes):
    flattened = routes.reshape(-1).astype(jnp.int32)
    member = (flattened[:, None] == jnp.arange(EXPERTS, dtype=jnp.int32)[None, :]).astype(jnp.int32)
    before = jnp.cumsum(member, axis=0) - member
    position = lax.optimization_barrier(jnp.sum(before * member, axis=1))
    return (flattened * CAP + position).astype(jnp.int32)

def normalize(tokens, gain_row):
    values = tokens.astype(jnp.float32)
    scaling = lax.rsqrt(lax.optimization_barrier(jnp.sum(values * values, axis=-1, keepdims=True)) / D + EPSILON)
    return (values, scaling, (values * scaling * gain_row).astype(jnp.bfloat16))

def gating(moe_in, router, routes):
    logits = jnp.dot(moe_in, router, preferred_element_type=jnp.float32)
    selection = (routes[:, :, None] == jnp.arange(EXPERTS, dtype=jnp.int32)[None, None, :]).astype(jnp.float32)
    chosen = lax.optimization_barrier(jnp.sum(logits[:, None, :] * selection, axis=-1))
    lifted = jax.nn.sigmoid(chosen)
    lifted_sum = lax.optimization_barrier(jnp.sum(lifted, axis=-1, keepdims=True))
    return (ROUTE_SCALE * lifted / lifted_sum, lifted, lifted_sum, selection)

def to_slots(rows, destination):
    filled = jnp.zeros((EXPERTS * CAP, rows.shape[-1]), rows.dtype).at[destination].set(rows)
    return filled.reshape(EXPERTS, CAP, rows.shape[-1])

def grouped_round(partial_value):
    rounded = lax.optimization_barrier(partial_value.astype(jnp.bfloat16))
    return lax.optimization_barrier(jnp.sum(rounded.astype(jnp.float32), axis=-2))

def up_project(buffer, gate_up):
    projected = jnp.einsum('ecd,edkf->eckf', buffer.astype(jnp.float32), gate_up.astype(jnp.float32))
    return (projected[:, :, 0], projected[:, :, 1])

def expert_forward(buffer, gate_up, down_w):
    gate_pre, second = up_project(buffer, gate_up)
    inner_act = (jax.nn.silu(gate_pre) * second).astype(jnp.bfloat16)
    group_width = FF // N_EXPERT
    split_inner = inner_act.reshape(EXPERTS, CAP, N_EXPERT, group_width).astype(jnp.float32)
    split_down = down_w.reshape(EXPERTS, N_EXPERT, group_width, D).astype(jnp.float32)
    partial_value = jnp.einsum('ecgf,egfd->ecgd', split_inner, split_down)
    return grouped_round(partial_value).astype(jnp.bfloat16)

def expert_backward(buffer, upstream, gate_up, down_w):
    gate_pre, second = up_project(buffer, gate_up)
    weighted = jnp.einsum('ecd,efd->ecf', upstream.astype(jnp.float32), down_w.astype(jnp.float32))
    lifted = jax.nn.sigmoid(gate_pre)
    activated = gate_pre * lifted
    inner_act = (activated * second).astype(jnp.bfloat16)
    gate_cot = lax.optimization_barrier(jnp.sum(inner_act.astype(jnp.float32) * weighted, axis=-1)).astype(jnp.bfloat16)
    grad_first = (weighted * second * lifted * (1.0 + gate_pre * (1.0 - lifted))).astype(jnp.bfloat16)
    grad_second = (weighted * activated).astype(jnp.bfloat16)
    stacked = jnp.stack([grad_first, grad_second], axis=2)
    group_width = FF // N_EXPERT
    split_grad = stacked.reshape(EXPERTS, CAP, 2, N_EXPERT, group_width).astype(jnp.float32)
    split_weight = gate_up.reshape(EXPERTS, D, 2, N_EXPERT, group_width).astype(jnp.float32)
    partial_value = jnp.einsum('eckgf,edkgf->ecgd', split_grad, split_weight)
    return (grouped_round(partial_value).astype(jnp.bfloat16), gate_cot)

def layer_forward(tokens, routes, gain_row, router, gate_up, down_w):
    values, scaling, moe_in = normalize(tokens, gain_row)
    gate_weights, lifted, lifted_sum, selection = gating(moe_in, router, routes)
    destination = slot_places(routes)
    buffer = to_slots(jnp.repeat(moe_in, TOPK, axis=0), destination)
    results = expert_forward(buffer, gate_up, down_w).reshape(EXPERTS * CAP, D)
    picked = jnp.take(results, destination, axis=0).reshape(TOK, TOPK, D)
    return (values + lax.optimization_barrier(jnp.sum(gate_weights[:, :, None] * picked.astype(jnp.float32), axis=1))).astype(jnp.bfloat16)

def layer_backward(stashed, incoming, routes, gain_row, router, gate_up, down_w):
    values, scaling, moe_in = normalize(stashed, gain_row)
    gate_weights, lifted, lifted_sum, selection = gating(moe_in, router, routes)
    destination = slot_places(routes)
    buffer = to_slots(jnp.repeat(moe_in, TOPK, axis=0), destination)
    upstream_slots = to_slots(jnp.repeat(incoming, TOPK, axis=0), destination)
    row_cot, gate_cot = expert_backward(buffer, upstream_slots, gate_up, down_w)
    back_rows = jnp.take(row_cot.reshape(EXPERTS * CAP, D), destination, axis=0).reshape(TOK, TOPK, D)
    back_gate = jnp.take(gate_cot.reshape(-1), destination, axis=0).reshape(TOK, TOPK).astype(jnp.float32)
    moe_cot = lax.optimization_barrier(jnp.sum(gate_weights[:, :, None] * back_rows.astype(jnp.float32), axis=1)).astype(jnp.bfloat16)
    mixed = lax.optimization_barrier(jnp.sum(back_gate * lifted, axis=-1, keepdims=True)) / lifted_sum
    chosen_cot = ROUTE_SCALE * (back_gate - mixed) / lifted_sum * lifted * (1.0 - lifted)
    logit_cot = lax.optimization_barrier(jnp.sum(chosen_cot[:, :, None] * selection, axis=1))
    norm_cot = moe_cot.astype(jnp.float32) + jnp.dot(logit_cot, router.astype(jnp.float32).T, precision=lax.Precision.HIGHEST)
    scaled = norm_cot * gain_row
    inner_product = lax.optimization_barrier(jnp.sum(scaled * values, axis=-1, keepdims=True))
    token_cot = incoming.astype(jnp.float32) + scaling * scaled - values * (scaling * scaling * scaling) * inner_product / D
    gain_cot = lax.optimization_barrier(jnp.sum(norm_cot * values * scaling, axis=0))
    return (token_cot.astype(jnp.bfloat16), gain_cot)

def reference(entering, pending, stashed_in, forward_routes, backward_routes, norm_gains, w_router, w_gateup, w_down):
    sequences = TOKENS // TOK

    def section_forward(operands):
        tokens, routes, gain_row, router, gate_up, down_w = operands

        def single(bundle):
            return layer_forward(bundle[0], bundle[1], gain_row, router, gate_up, down_w)
        done = lax.map(single, (tokens.reshape(sequences, TOK, D), routes.reshape(sequences, TOK, TOPK)))
        return done.reshape(TOKENS, D)

    def section_backward(operands):
        stashed, incoming, routes, gain_row, router, gate_up, down_w = operands

        def single(bundle):
            return layer_backward(bundle[0], bundle[1], bundle[2], gain_row, router, gate_up, down_w)
        cotangents, gain_parts = lax.map(single, (stashed.reshape(sequences, TOK, D), incoming.reshape(sequences, TOK, D), routes.reshape(sequences, TOK, TOPK)))
        return (cotangents.reshape(TOKENS, D), lax.optimization_barrier(jnp.sum(gain_parts, axis=0)))
    produced = lax.map(section_forward, (entering, forward_routes, norm_gains, w_router, w_gateup, w_down))
    cotangents, gain_grads = lax.map(section_backward, (stashed_in, pending, backward_routes, norm_gains, w_router, w_gateup, w_down))
    passed_forward = jnp.concatenate([jnp.zeros_like(produced[:1]), produced[:-1]], axis=0)
    passed_backward = jnp.concatenate([cotangents[1:], jnp.zeros_like(cotangents[:1])], axis=0)
    return (produced, cotangents, passed_forward, passed_backward, gain_grads)
```

```python
import functools

import jax
import jax.numpy as jnp
from jax import lax
from jax.experimental import pallas as pl
from jax.experimental.pallas import tpu as pltpu
from jax.sharding import PartitionSpec as P

ROUTE_SCALE = 2.827
EPSILON = 1e-05
F32 = jnp.float32
BF16 = jnp.bfloat16
MESH = pl.DeviceIdType.MESH
NT = (((1,), (1,)), ((), ()))
GAIN_ROW = 7


def nt(a, b):
    return lax.dot_general(a, b, NT, preferred_element_type=F32)


def nn(a, b):
    return jnp.dot(a, b, preferred_element_type=F32)


def split(v):
    hi = v.astype(BF16)
    return hi, (v - hi.astype(F32)).astype(BF16)


def kernel(
    cfg,
    xb_in, gy_in, xf_in, routes_in, small_in, wgu_in, wd_in,
    fo, ig, pf, pb, gg,
    g_all, rt, sm, wgu, wd, rows_x, rows_g, acc_a, acc_b, acc_w, inner, grad,
    ret_send, ret, comb_send, comb, own, hot, wts, gs, gr, dm, ip, gpart, r_tok, rpad,
    send_sem, recv_sem, local_sem,
):
    NP, ND, NY, TOK, DL, FFL, K, E, CAP = cfg
    HT = TOK // 2
    W = min(256, DL)
    tiles = DL // W
    NSLOT = E * CAP
    D = DL * NY
    p, d, y = lax.axis_index("pipe"), lax.axis_index("dp"), lax.axis_index("expert")
    core = lax.rem(d, 2)
    mate = d + 1 - 2 * core
    across = [lax.rem(d + 2 * o, ND) for o in range(1, ND // 2)]
    others_y = [lax.rem(y + o, NY) for o in range(1, NY)]
    others_d = [lax.rem(d + o, ND) for o in range(1, ND)]
    up, down = lax.rem(p + 1, NP), lax.rem(p + NP - 1, NP)

    counter = {"s": 0, "r": 0, "l": 0}
    pending = []

    def remote(src, dst, r_index, where):
        i = counter["s"]
        counter["s"] += 1
        c = pltpu.make_async_remote_copy(
            src_ref=src, dst_ref=dst, send_sem=send_sem.at[i], recv_sem=recv_sem.at[r_index],
            device_id=where, device_id_type=MESH,
        )
        c.start()
        pending.append(c)

    def arrived(ref, r_index):
        pltpu.make_async_remote_copy(
            src_ref=ref, dst_ref=ref, send_sem=send_sem.at[0], recv_sem=recv_sem.at[r_index],
            device_id=(p, d, y), device_id_type=MESH,
        ).wait_recv()

    def local(src, dst):
        i = counter["l"]
        counter["l"] += 1
        c = pltpu.make_async_copy(src, dst, local_sem.at[i])
        c.start()
        return c

    def block(n):
        base = counter["r"]
        counter["r"] += n
        return base

    first = [local(src, g_all.at[t, d, y]) for t, src in enumerate((xb_in, gy_in, xf_in))]
    first.append(local(routes_in, rt.at[d]))
    first.append(local(small_in, sm.at[y]))
    weights = [local(wgu_in.at[k, pl.ds(j * DL, DL)], wgu.at[k, j]) for k in range(2) for j in range(NY)]
    weights += [local(wd_in.at[:, pl.ds(j * DL, DL)], wd.at[j]) for j in range(NY)]

    barrier = pltpu.get_barrier_semaphore()
    for o in range(ND):
        for v in range(NY):
            if o or v:
                pl.semaphore_signal(
                    barrier, inc=1, device_id=(p, lax.rem(d + o, ND), lax.rem(y + v, NY)), device_id_type=MESH
                )
    pl.semaphore_signal(barrier, inc=1, device_id=(up, d, y), device_id_type=MESH)
    pl.semaphore_signal(barrier, inc=1, device_id=(down, d, y), device_id_type=MESH)
    pl.semaphore_wait(barrier, ND * NY + 1)
    for c in first:
        c.wait()

    gbase = block(3 * ND * NY * 2)

    def piece(t, dd, yy, h):
        return g_all.at[t, dd, yy, pl.ds(h * HT, HT)]

    def gsem(t, dd, yy, h):
        return gbase + ((t * ND + dd) * NY + yy) * 2 + h

    def gsend(t, dd, yy, h, where):
        ref = piece(t, dd, yy, h)
        remote(ref, ref, gsem(t, dd, yy, h), where)

    def gwait(t, dd, yy, h):
        arrived(piece(t, dd, yy, h), gsem(t, dd, yy, h))

    def send_own(t):
        for i in range(2):
            for x in across:
                gsend(t, d, y, i, (p, x, y))
            for v in others_y:
                gsend(t, d, y, 1 - i, (p, d, v))
        for i in range(2):
            gsend(t, d, y, i, (p, mate, y))

    def relay(t):
        for i in range(2):
            for x in across:
                gwait(t, x, y, i)
                if i == 0:
                    for v in others_y:
                        gsend(t, x, y, 0, (p, d, v))
                gsend(t, x, y, i, (p, mate, y))
            for v in others_y:
                gwait(t, d, v, 1 - i)
                if i == 0:
                    for x in across:
                        gsend(t, d, v, 1, (p, x, y))
                gsend(t, d, v, 1 - i, (p, mate, y))

    def finish(t):
        for x in across:
            for v in others_y:
                for h in range(2):
                    gwait(t, x, v, h)
                    gsend(t, x, v, h, (p, mate, y))
        for dd in [mate] + [lax.rem(mate + 2 * o, ND) for o in range(1, ND // 2)]:
            for v in range(NY):
                for h in range(2):
                    gwait(t, dd, v, h)

    rbase, sbase = block(ND), block(NY)
    for s in others_d:
        remote(rt.at[d], rt.at[d], rbase + d, (p, s, y))
    for v in others_y:
        remote(sm.at[y], sm.at[y], sbase + y, (p, d, v))
    send_own(0)
    send_own(1)
    for s in others_d:
        arrived(rt.at[s], rbase + s)
    for v in others_y:
        arrived(sm.at[v], sbase + v)

    before = (
        lax.broadcasted_iota(jnp.int32, (TOK, TOK), 0) < lax.broadcasted_iota(jnp.int32, (TOK, TOK), 1)
    ).astype(F32).astype(BF16)
    row8 = lax.broadcasted_iota(jnp.int32, (8, TOK), 0)
    slot = lax.broadcasted_iota(jnp.int32, (CAP, TOK), 0).astype(F32)

    def one_hot(member_row, pos_row):
        return jnp.where(slot == pos_row, member_row, 0.0)

    def expert_hot(s, base):
        picks = rt[s]
        member = jnp.zeros((8, TOK), F32)
        for k in range(K):
            member += (picks[base + k : base + k + 1, :] == d).astype(F32)
        pos = nn(member.astype(BF16), before)
        return one_hot(member[0:1, :], pos[0:1, :]).astype(BF16)

    def dispatch(t, base, rows, scaled):
        def body(s, _):
            pick = expert_hot(s, base)
            where = pl.ds(pl.multiple_of(s * CAP, CAP), CAP)
            total = jnp.zeros((CAP, 1), F32)
            for j in range(NY):
                def step(i, tot, j=j):
                    cols = pl.ds(pl.multiple_of(i * W, W), W)
                    part = nn(pick, g_all[t, s, j, :, cols])
                    rows[j, where, cols] = part.astype(BF16)
                    return tot + jnp.sum(part * part, axis=-1, keepdims=True)

                total = lax.fori_loop(0, tiles, step, total)
            if scaled:
                scaling = lax.rsqrt(total / D + EPSILON)
                for j in range(NY):
                    def norm(i, c, j=j):
                        cols = pl.ds(pl.multiple_of(i * W, W), W)
                        v = rows[j, where, cols].astype(F32) * scaling * sm[j, GAIN_ROW : GAIN_ROW + 1, cols]
                        rows[j, where, cols] = v.astype(BF16)
                        return c

                    lax.fori_loop(0, tiles, norm, 0)
            return 0

        lax.fori_loop(0, ND, body, 0)

    def project_up():
        acc_a[...] = jnp.zeros_like(acc_a)
        acc_b[...] = jnp.zeros_like(acc_b)
        KT = min(512, DL)
        for j in range(NY):
            def body(i, c, j=j):
                ks = pl.ds(pl.multiple_of(i * KT, KT), KT)
                lhs = rows_x[j, :, ks]
                acc_a[...] += nn(lhs, wgu[0, j, ks, :])
                acc_b[...] += nn(lhs, wgu[1, j, ks, :])
                return c

            lax.fori_loop(0, DL // KT, body, 0)

    def project_w():
        acc_w[...] = jnp.zeros_like(acc_w)
        KT = min(512, DL)
        for j in range(NY):
            def body(i, c, j=j):
                ks = pl.ds(pl.multiple_of(i * KT, KT), KT)
                acc_w[...] += nt(rows_g[j, :, ks], wd[j, :, ks])
                return c

            lax.fori_loop(0, DL // KT, body, 0)

    def owner(t, base, u):
        def squares(j, tot):
            def step(i, tt):
                v = g_all[t, d, j, :, pl.ds(pl.multiple_of(i * W, W), W)].astype(F32)
                return tt + jnp.sum(v * v, axis=-1, keepdims=True)

            return lax.fori_loop(0, tiles, step, tot)

        total = lax.fori_loop(0, NY, squares, jnp.zeros((TOK, 1), F32))
        scaling = lax.rsqrt(total / D + EPSILON)

        def logit(j, acc):
            def step(i, a):
                cols = pl.ds(pl.multiple_of(i * W, W), W)
                v = g_all[t, d, j, :, cols].astype(F32) * scaling * sm[j, GAIN_ROW : GAIN_ROW + 1, cols]
                return a + nt(sm[j, :, cols].astype(BF16), v.astype(BF16))

            return lax.fori_loop(0, tiles, step, acc)

        logits = lax.fori_loop(0, NY, logit, jnp.zeros((8, TOK), F32))
        picks = rt[d]
        sel = jnp.zeros((8, TOK), F32)
        for k in range(K):
            sel += (picks[base + k : base + k + 1, :] == row8).astype(F32)
        pos = nn(sel.astype(BF16), before)
        sg = jnp.where(sel > 0.5, jax.nn.sigmoid(logits), 0.0)
        total_sg = jnp.sum(sg, axis=0, keepdims=True)
        gate = ROUTE_SCALE * sg / total_sg
        weighted = []
        for e in range(E):
            h = one_hot(sel[e : e + 1, :], pos[e : e + 1, :])
            hot[u, e] = h.astype(BF16)
            weighted.append(h * gate[e : e + 1, :])
        g = jnp.transpose(jnp.concatenate(weighted, axis=0))
        hi, lo = split(g)
        wts[u, 0] = hi
        wts[u, 1] = lo
        return scaling, sel, sg, total_sg

    retbase = [block(NY * ND) for _ in range(2)]
    cbase = [block(NY) for _ in range(2)]
    gcbase, ipbase, gpbase, zbase = block(ND * NY), block(NY), block(ND), block(2)

    def chunk_of(i):
        return lax.rem(y + 1 + i, NY)

    def produce(u, i, make):
        j = chunk_of(i)

        def body(n, c):
            cols = pl.ds(pl.multiple_of(n * W, W), W)
            ret_send[u, j, :, :, cols] = make(j, cols).astype(BF16).reshape(ND, CAP, W)
            return c

        lax.fori_loop(0, tiles, body, 0)
        for s in others_d:
            remote(ret_send.at[u, j, s], ret.at[u, j, d], retbase[u] + j * ND + d, (p, s, y))
        return local(ret_send.at[u, j, d], ret.at[u, j, d])

    def combine(u, i, kept):
        j = chunk_of(i)
        for s in others_d:
            arrived(ret.at[u, j, s], retbase[u] + j * ND + s)
        kept.wait()

        def body(n, c):
            cols = pl.ds(pl.multiple_of(n * W, W), W)
            r = ret[u, j, :, :, cols].reshape(NSLOT, W)
            v = nn(wts[u, 0], r) + nn(wts[u, 1], r)
            if i < NY - 1:
                comb_send[u, j, :, cols] = v.astype(BF16)
            else:
                own[:, cols] = v
            return c

        lax.fori_loop(0, tiles, body, 0)
        if i < NY - 1:
            remote(comb_send.at[u, j], comb.at[u, y], cbase[u] + y, (p, d, j))

    def combined(u, cols):
        v = own[:, cols]
        for w in others_y:
            v = v + comb[u, w, :, cols].astype(F32)
        return v

    relay(0)
    relay(1)
    send_own(2)
    r_b, sel_b, sg_b, sum_b = owner(0, K, 0)
    r_tok[...] = jnp.broadcast_to(r_b, r_tok.shape)
    finish(0)
    dispatch(0, K, rows_x, True)
    for c in weights:
        c.wait()
    project_up()
    finish(1)
    dispatch(1, K, rows_g, False)
    project_w()
    ones8 = jnp.ones((8, FFL), BF16)

    def activate(s, c):
        where = pl.ds(pl.multiple_of(s * CAP, CAP), CAP)
        a, b, w = acc_a[where, :], acc_b[where, :], acc_w[where, :]
        sa = jax.nn.sigmoid(a)
        act = a * sa
        prod = (act * b).astype(BF16).astype(F32) * w
        hi, lo = split(prod)
        gs[s] = nt(ones8, hi) + nt(ones8, lo)
        grad[0, where, :] = (w * b * sa * (1.0 + a * (1.0 - sa))).astype(BF16)
        grad[1, where, :] = (w * act).astype(BF16)
        return c

    lax.fori_loop(0, ND, activate, 0)
    for o in range(ND):
        for v in range(NY):
            if o or v:
                s = lax.rem(d + o, ND)
                remote(gs.at[s], gr.at[d, y], gcbase + d * NY + y, (p, s, lax.rem(y + v, NY)))
    kept_gc = local(gs.at[d], gr.at[d, y])

    def back_rows(j, cols):
        return nt(grad[0], wgu[0, j, cols, :]) + nt(grad[1], wgu[1, j, cols, :])

    relayed = False
    kept_b = []
    for i in range(NY):
        kept_b.append(produce(0, i, back_rows))
        if i == 0:
            relay(2)
    owner(2, 0, 1)
    finish(2)
    dispatch(2, 0, rows_x, True)
    project_up()

    def act_forward(s, c):
        where = pl.ds(pl.multiple_of(s * CAP, CAP), CAP)
        a, b = acc_a[where, :], acc_b[where, :]
        inner[where, :] = (a * jax.nn.sigmoid(a) * b).astype(BF16)
        return c

    lax.fori_loop(0, ND, act_forward, 0)

    def forward_rows(j, cols):
        return nn(inner[...], wd[j, :, cols])

    kept_f = []
    for i in range(NY):
        combine(0, i, kept_b[i])
        kept_f.append(produce(1, i, forward_rows))

    kept_gc.wait()
    for o in range(ND):
        for v in range(NY):
            if o or v:
                s, w = lax.rem(d + o, ND), lax.rem(y + v, NY)
                arrived(gr.at[s, w], gcbase + s * NY + w)
    gc = jnp.zeros((8, TOK), F32)
    for e in range(E):
        t = gr[e, 0]
        for v in range(1, NY):
            t = t + gr[e, v]
        gc = gc + jnp.where(row8 == e, nn(t.astype(BF16), hot[0, e]), 0.0)
    mixed = jnp.sum(gc * sg_b, axis=0, keepdims=True) / sum_b
    dl = jnp.where(sel_b > 0.5, ROUTE_SCALE * (gc - mixed) / sum_b * sg_b * (1.0 - sg_b), 0.0)
    dl_hi, dl_lo = split(jnp.transpose(jnp.concatenate([dl, jnp.zeros((TOK - 8, TOK), F32)], axis=0)))
    rpad[...] = jnp.zeros_like(rpad)
    rpad[0:8, :] = sm[y]
    for w in others_y:
        arrived(comb.at[0, w], cbase[0] + w)

    def tail_one(n, tot):
        cols = pl.ds(pl.multiple_of(n * W, W), W)
        router = rpad[:, cols].astype(BF16)
        moe = combined(0, cols).astype(BF16).astype(F32)
        v = moe + nn(dl_hi, router) + nn(dl_lo, router)
        dm[:, cols] = v
        x = g_all[0, d, y, :, cols].astype(F32)
        gpart[d, :, cols] = jnp.sum(v * x * r_tok[:, 0:1], axis=0, keepdims=True)
        return tot + jnp.sum(v * sm[y, GAIN_ROW : GAIN_ROW + 1, cols] * x, axis=-1, keepdims=True)

    part = lax.fori_loop(0, tiles, tail_one, jnp.zeros((TOK, 1), F32))
    ip[y] = jnp.broadcast_to(part, (TOK, 128))
    for v in others_y:
        remote(ip.at[y], ip.at[y], ipbase + y, (p, d, v))
    for s in others_d:
        remote(gpart.at[d], gpart.at[d], gpbase + d, (p, s, y))
    for v in others_y:
        arrived(ip.at[v], ipbase + v)
    inner_sum = ip[0]
    for v in range(1, NY):
        inner_sum = inner_sum + ip[v]
    inner_sum = inner_sum[:, 0:1]

    def tail_two(n, c):
        cols = pl.ds(pl.multiple_of(n * W, W), W)
        r = r_tok[:, 0:1]
        h = dm[:, cols] * sm[y, GAIN_ROW : GAIN_ROW + 1, cols]
        x = g_all[0, d, y, :, cols].astype(F32)
        g = g_all[1, d, y, :, cols].astype(F32)
        ig[:, cols] = (g + r * h - x * (r * r * r) * inner_sum / D).astype(BF16)
        return c

    lax.fori_loop(0, tiles, tail_two, 0)

    def hand_on(src, dst, which, has, gets, where):
        i = counter["s"]
        counter["s"] += 1
        c = pltpu.make_async_remote_copy(
            src_ref=src, dst_ref=dst, send_sem=send_sem.at[i], recv_sem=recv_sem.at[zbase + which],
            device_id=where, device_id_type=MESH,
        )

        @pl.when(has)
        def _():
            c.start()

        @pl.when(jnp.logical_not(gets))
        def _():
            dst[...] = jnp.zeros_like(dst)

        def done():
            @pl.when(has)
            def _():
                c.wait_send()

            @pl.when(gets)
            def _():
                c.wait_recv()

        return done

    done_b = hand_on(ig, pb, 0, p > 0, p < NP - 1, (down, d, y))

    for i in range(NY):
        combine(1, i, kept_f[i])
    for w in others_y:
        arrived(comb.at[1, w], cbase[1] + w)

    def out_tile(n, c):
        cols = pl.ds(pl.multiple_of(n * W, W), W)
        fo[:, cols] = (g_all[2, d, y, :, cols].astype(F32) + combined(1, cols)).astype(BF16)
        return c

    lax.fori_loop(0, tiles, out_tile, 0)
    done_f = hand_on(fo, pf, 1, p < NP - 1, p > 0, (up, d, y))

    for s in others_d:
        arrived(gpart.at[s], gpbase + s)
    total = gpart[0]
    for s in range(1, ND):
        total = total + gpart[s]
    gg[...] = total
    for c in pending:
        c.wait_send()
    done_b()
    done_f()


def local(mesh_sizes, entering, pending, stashed_in, forward_routes, backward_routes, norm_gains, w_router, w_gateup, w_down):
    NP, ND, NY = mesh_sizes
    _, TOK, DL = entering.shape
    K = forward_routes.shape[2]
    E = w_router.shape[2]
    FFL = w_gateup.shape[4]
    D = w_gateup.shape[2]
    CAP = TOK * K // E
    assert E == ND and E <= GAIN_ROW and 2 * K <= 8 and D == DL * NY
    routes = jnp.concatenate([forward_routes[0].T, backward_routes[0].T], axis=0)
    routes = jnp.pad(routes, ((0, 8 - 2 * K), (0, 0)), constant_values=-1)
    small = jnp.concatenate(
        [w_router[0].T.astype(F32), jnp.zeros((GAIN_ROW - E, DL), F32), norm_gains[0][None]], axis=0
    )
    wgu = jnp.transpose(w_gateup[0, 0], (1, 0, 2))
    cfg = (NP, ND, NY, TOK, DL, FFL, K, E, CAP)
    NS = E * CAP
    nsend = 3 * (2 * (ND // 2 + NY) * 4 + 4 * ND * NY) + 8 * ND * NY + 64
    nrecv = 3 * ND * NY * 2 + 3 * ND * NY + 4 * ND + 6 * NY + 16
    out = jax.ShapeDtypeStruct((TOK, DL), BF16)
    V = pltpu.VMEM
    res = pl.pallas_call(
        functools.partial(kernel, cfg),
        out_shape=[out, out, out, out, jax.ShapeDtypeStruct((1, DL), F32)],
        in_specs=[pl.BlockSpec(memory_space=pl.ANY)] * 7,
        out_specs=[pl.BlockSpec(memory_space=pltpu.VMEM)] * 5,
        scratch_shapes=[
            V((3, ND, NY, TOK, DL), BF16),
            V((ND, 8, TOK), jnp.int32),
            V((NY, 8, DL), F32),
            V((2, NY, DL, FFL), BF16),
            V((NY, FFL, DL), BF16),
            V((NY, NS, DL), BF16),
            V((NY, NS, DL), BF16),
            V((NS, FFL), F32),
            V((NS, FFL), F32),
            V((NS, FFL), F32),
            V((NS, FFL), BF16),
            V((2, NS, FFL), BF16),
            V((2, NY, ND, CAP, DL), BF16),
            V((2, NY, ND, CAP, DL), BF16),
            V((2, NY, TOK, DL), BF16),
            V((2, NY, TOK, DL), BF16),
            V((TOK, DL), F32),
            V((2, E, CAP, TOK), BF16),
            V((2, 2, TOK, NS), BF16),
            V((ND, 8, CAP), F32),
            V((ND, NY, 8, CAP), F32),
            V((TOK, DL), F32),
            V((NY, TOK, 128), F32),
            V((ND, 1, DL), F32),
            V((TOK, 128), F32),
            V((TOK, DL), F32),
            pltpu.SemaphoreType.DMA((nsend,)),
            pltpu.SemaphoreType.DMA((nrecv,)),
            pltpu.SemaphoreType.DMA((64,)),
        ],
        compiler_params=pltpu.CompilerParams(
            collective_id=0, has_side_effects=True, vmem_limit_bytes=62 * 1024 * 1024
        ),
    )(stashed_in[0], pending[0], entering[0], routes, small, wgu, w_down[0, 0])
    fo, ig, pf, pb, gg = res
    return fo[None], ig[None], pf[None], pb[None], gg


def solution(mesh):
    tokens = P("pipe", "dp", "expert")
    placed = (
        tokens, tokens, tokens,
        P("pipe", "dp", None), P("pipe", "dp", None),
        P("pipe", "expert"), P("pipe", "expert", None),
        P("pipe", "dp", None, None, "expert"), P("pipe", "dp", "expert", None),
    )
    sizes = tuple(mesh.shape[a] for a in ("pipe", "dp", "expert"))
    return jax.shard_map(
        functools.partial(local, sizes),
        mesh=mesh,
        in_specs=placed,
        out_specs=(tokens, tokens, tokens, tokens, P("pipe", "expert")),
        check_vma=False,
    )
```

```python
import functools

import jax
import jax.numpy as jnp
from jax import lax
from jax.experimental import pallas as pl
from jax.experimental.pallas import tpu as pltpu
from jax.sharding import PartitionSpec as P

ROUTE_SCALE = 2.827
EPSILON = 1e-05
F32 = jnp.float32
BF16 = jnp.bfloat16
MESH = pl.DeviceIdType.MESH
NT = (((1,), (1,)), ((), ()))
GAIN_ROW = 7


def nt(a, b):
    return lax.dot_general(a, b, NT, preferred_element_type=F32)


def nn(a, b):
    return jnp.dot(a, b, preferred_element_type=F32)


def split(v):
    hi = v.astype(BF16)
    return hi, (v - hi.astype(F32)).astype(BF16)


def settle(*refs):
    sources, targets, held, sem = refs[:5], refs[5:10], refs[10:15], refs[15]
    into = [pltpu.make_async_copy(a, b, sem.at[i]) for i, (a, b) in enumerate(zip(sources, held))]
    out = [pltpu.make_async_copy(a, b, sem.at[5 + i]) for i, (a, b) in enumerate(zip(held, targets))]
    for c in into:
        c.start()
    for a, b in zip(into, out):
        a.wait()
        b.start()
    for c in out:
        c.wait()


def lanes(v):
    total = v[:, 0:128]
    for i in range(1, v.shape[1] // 128):
        total = total + v[:, i * 128 : (i + 1) * 128]
    return total


def kernel(
    cfg,
    xb_in, gy_in, xf_in, wgu_in, wd_in, fr_in, br_in, router_in, gain_in,
    fo, ig, pf, pb, gg,
    g_all, rt, sm, wgu, wd, rows_x, rows_g, acc_a, acc_b, acc_w, inner, grad,
    ret_send, ret, comb_send, comb, own, hot, wts, gs, gr, dm, ip, gpart, r_tok, rpad, r_row,
    send_sem, recv_sem, local_sem,
):
    NP, ND, NY, TOK, DL, FFL, K, E, CAP = cfg
    HT = TOK // 2
    W = min(256, DL)
    tiles = DL // W
    BW = min(512, DL // 2)
    HALF = DL // 2
    NSLOT = E * CAP
    D = DL * NY
    p, d, y = lax.axis_index("pipe"), lax.axis_index("dp"), lax.axis_index("expert")
    core = lax.rem(d, 2)
    mate = d + 1 - 2 * core
    across = [lax.rem(d + 2 * o, ND) for o in range(1, ND // 2)]
    others_y = [lax.rem(y + o, NY) for o in range(1, NY)]
    others_d = [lax.rem(d + o, ND) for o in range(1, ND)]
    up, down = lax.rem(p + 1, NP), lax.rem(p + NP - 1, NP)

    counter = {"s": 0, "r": 0, "l": 0}
    pending = []

    def remote(src, dst, r_index, where):
        i = counter["s"]
        counter["s"] += 1
        c = pltpu.make_async_remote_copy(
            src_ref=src, dst_ref=dst, send_sem=send_sem.at[i], recv_sem=recv_sem.at[r_index],
            device_id=where, device_id_type=MESH,
        )
        c.start()
        pending.append(c)

    def arrived(ref, r_index):
        pltpu.make_async_remote_copy(
            src_ref=ref, dst_ref=ref, send_sem=send_sem.at[0], recv_sem=recv_sem.at[r_index],
            device_id=(p, d, y), device_id_type=MESH,
        ).wait_recv()

    def local(src, dst):
        i = counter["l"]
        counter["l"] += 1
        c = pltpu.make_async_copy(src, dst, local_sem.at[i])
        c.start()
        return c

    def block(n):
        base = counter["r"]
        counter["r"] += n
        return base

    first = [local(src, g_all.at[t, d, y]) for t, src in enumerate((xb_in, gy_in, xf_in))]
    rt[d] = jnp.full((8, TOK), -1, jnp.int32)
    rt[d, 0:K, :] = fr_in[...]
    rt[d, K : 2 * K, :] = br_in[...]
    sm[y] = jnp.zeros((8, DL), F32)
    sm[y, 0:E, :] = router_in[...].astype(F32)
    sm[y, GAIN_ROW : GAIN_ROW + 1, :] = gain_in[...]
    weights = [local(wgu_in.at[k, pl.ds(j * DL, DL)], wgu.at[k, j]) for k in range(2) for j in range(NY)]
    weights += [local(wd_in.at[:, pl.ds(j * DL, DL)], wd.at[j]) for j in range(NY)]

    barrier = pltpu.get_barrier_semaphore()
    for o in range(ND):
        for v in range(NY):
            if o or v:
                pl.semaphore_signal(
                    barrier, inc=1, device_id=(p, lax.rem(d + o, ND), lax.rem(y + v, NY)), device_id_type=MESH
                )
    pl.semaphore_signal(barrier, inc=1, device_id=(up, d, y), device_id_type=MESH)
    pl.semaphore_signal(barrier, inc=1, device_id=(down, d, y), device_id_type=MESH)
    pl.semaphore_wait(barrier, ND * NY + 1)
    for c in first:
        c.wait()

    gbase = block(3 * ND * NY * 2)

    def piece(t, dd, yy, h):
        return g_all.at[t, dd, yy, pl.ds(h * HT, HT)]

    def gsem(t, dd, yy, h):
        return gbase + ((t * ND + dd) * NY + yy) * 2 + h

    def gsend(t, dd, yy, h, where):
        ref = piece(t, dd, yy, h)
        remote(ref, ref, gsem(t, dd, yy, h), where)

    def gwait(t, dd, yy, h):
        arrived(piece(t, dd, yy, h), gsem(t, dd, yy, h))

    def send_own(t):
        for i in range(2):
            for x in across:
                gsend(t, d, y, i, (p, x, y))
            for v in others_y:
                gsend(t, d, y, 1 - i, (p, d, v))
        for i in range(2):
            gsend(t, d, y, i, (p, mate, y))

    def relay(t):
        for i in range(2):
            for x in across:
                gwait(t, x, y, i)
                if i == 0:
                    for v in others_y:
                        gsend(t, x, y, 0, (p, d, v))
                gsend(t, x, y, i, (p, mate, y))
            for v in others_y:
                gwait(t, d, v, 1 - i)
                if i == 0:
                    for x in across:
                        gsend(t, d, v, 1, (p, x, y))
                gsend(t, d, v, 1 - i, (p, mate, y))

    def finish(t):
        for x in across:
            for v in others_y:
                for h in range(2):
                    gwait(t, x, v, h)
                    gsend(t, x, v, h, (p, mate, y))
        for dd in [mate] + [lax.rem(mate + 2 * o, ND) for o in range(1, ND // 2)]:
            for v in range(NY):
                for h in range(2):
                    gwait(t, dd, v, h)

    rbase, sbase = block(ND), block(NY)
    for s in others_d:
        remote(rt.at[d], rt.at[d], rbase + d, (p, s, y))
    for v in others_y:
        remote(sm.at[y], sm.at[y], sbase + y, (p, d, v))
    send_own(0)
    send_own(1)
    for s in others_d:
        arrived(rt.at[s], rbase + s)
    for v in others_y:
        arrived(sm.at[v], sbase + v)

    before = (
        lax.broadcasted_iota(jnp.int32, (TOK, TOK), 0) < lax.broadcasted_iota(jnp.int32, (TOK, TOK), 1)
    ).astype(F32).astype(BF16)
    row8 = lax.broadcasted_iota(jnp.int32, (8, TOK), 0)
    slot = lax.broadcasted_iota(jnp.int32, (CAP, TOK), 0).astype(F32)

    def one_hot(member_row, pos_row):
        return jnp.where(slot == pos_row, member_row, 0.0)

    def expert_hot(s, base):
        picks = rt[s]
        member = jnp.zeros((8, TOK), F32)
        for k in range(K):
            member += (picks[base + k : base + k + 1, :] == d).astype(F32)
        pos = nn(member.astype(BF16), before)
        return one_hot(member[0:1, :], pos[0:1, :]).astype(BF16)

    def dispatch(t, base, rows, scaled):
        PW = min(512, DL)

        def body(s, _):
            pick = expert_hot(s, base)
            where = pl.ds(pl.multiple_of(s * CAP, CAP), CAP)
            total = jnp.zeros((CAP, 128), F32)
            for j in range(NY):
                for i in range(DL // PW):
                    cols = pl.ds(i * PW, PW)
                    part = nn(pick, g_all[t, s, j, :, cols])
                    if scaled:
                        total = total + lanes(part * part)
                        part = part * sm[j, GAIN_ROW : GAIN_ROW + 1, cols]
                    rows[j, where, cols] = part.astype(BF16)
            if scaled:
                scaling = lax.rsqrt(jnp.sum(total, axis=-1, keepdims=True) / D + EPSILON)
                r_row[where, :] = jnp.broadcast_to(scaling, (CAP, 128))
            return 0

        lax.fori_loop(0, ND, body, 0)

    def project_up():
        acc_a[...] = jnp.zeros_like(acc_a)
        acc_b[...] = jnp.zeros_like(acc_b)
        KT = min(1024, DL)
        for j in range(NY):
            def body(i, c, j=j):
                ks = pl.ds(pl.multiple_of(i * KT, KT), KT)
                lhs = rows_x[j, :, ks]
                acc_a[...] += nn(lhs, wgu[0, j, ks, :])
                acc_b[...] += nn(lhs, wgu[1, j, ks, :])
                return c

            lax.fori_loop(0, DL // KT, body, 0)

    def project_w():
        acc_w[...] = jnp.zeros_like(acc_w)
        KT = min(1024, DL)
        for j in range(NY):
            def body(i, c, j=j):
                ks = pl.ds(pl.multiple_of(i * KT, KT), KT)
                acc_w[...] += nt(rows_g[j, :, ks], wd[j, :, ks])
                return c

            lax.fori_loop(0, DL // KT, body, 0)

    def owner(t, base, u):
        def squares(j, tot):
            def step(i, tt):
                v = g_all[t, d, j, :, pl.ds(pl.multiple_of(i * W, W), W)].astype(F32)
                return tt + lanes(v * v)

            return lax.fori_loop(0, tiles, step, tot, unroll=2)

        total = lax.fori_loop(0, NY, squares, jnp.zeros((TOK, 128), F32))
        total = jnp.sum(total, axis=-1, keepdims=True)
        scaling = lax.rsqrt(total / D + EPSILON)

        def logit(j, acc):
            def step(i, a):
                cols = pl.ds(pl.multiple_of(i * W, W), W)
                v = g_all[t, d, j, :, cols].astype(F32) * scaling * sm[j, GAIN_ROW : GAIN_ROW + 1, cols]
                return a + nt(sm[j, :, cols].astype(BF16), v.astype(BF16))

            return lax.fori_loop(0, tiles, step, acc, unroll=2)

        logits = lax.fori_loop(0, NY, logit, jnp.zeros((8, TOK), F32))
        picks = rt[d]
        sel = jnp.zeros((8, TOK), F32)
        for k in range(K):
            sel += (picks[base + k : base + k + 1, :] == row8).astype(F32)
        pos = nn(sel.astype(BF16), before)
        sg = jnp.where(sel > 0.5, jax.nn.sigmoid(logits), 0.0)
        total_sg = jnp.sum(sg, axis=0, keepdims=True)
        gate = ROUTE_SCALE * sg / total_sg
        weighted = []
        for e in range(E):
            h = one_hot(sel[e : e + 1, :], pos[e : e + 1, :])
            hot[u, e] = h.astype(BF16)
            weighted.append(h * gate[e : e + 1, :])
        g = jnp.transpose(jnp.concatenate(weighted, axis=0))
        hi, lo = split(g)
        wts[u, 0] = hi
        wts[u, 1] = lo
        return scaling, sel, sg, total_sg

    retbase = [block(NY * ND * 2) for _ in range(2)]
    cbase = [block(2 * NY) for _ in range(2)]
    gcbase, ipbase, gpbase, zbase = block(ND * NY), block(NY), block(ND), block(3)

    def chunk_of(i):
        return lax.rem(y + 1 + i, NY)

    def back(ref, u, j, s, h):
        return ref.at[u, j, s, :, pl.ds(h * HALF, HALF)]

    def produce(u, i, h, make):
        j = chunk_of(i)

        def body(n, c):
            cols = pl.ds(pl.multiple_of(h * HALF + n * BW, BW), BW)
            ret_send[u, j, :, :, cols] = make(j, cols).astype(BF16).reshape(ND, CAP, BW)
            return c

        lax.fori_loop(0, HALF // BW, body, 0, unroll=True)
        for s in others_d:
            remote(back(ret_send, u, j, s, h), back(ret, u, j, d, h), retbase[u] + (j * ND + d) * 2 + h, (p, s, y))
        return local(back(ret_send, u, j, d, h), back(ret, u, j, d, h))

    def combine(u, i, h, kept):
        j = chunk_of(i)
        for s in others_d:
            arrived(back(ret, u, j, s, h), retbase[u] + (j * ND + s) * 2 + h)
        kept.wait()

        def body(n, c):
            cols = pl.ds(pl.multiple_of(h * HALF + n * BW, BW), BW)
            r = ret[u, j, :, :, cols].reshape(NSLOT, BW)
            v = nn(wts[u, 0], r) + nn(wts[u, 1], r)
            if i < NY - 1:
                comb_send[u, j, :, cols] = v.astype(BF16)
            else:
                own[:, cols] = v
            return c

        lax.fori_loop(0, HALF // BW, body, 0, unroll=True)
        if i < NY - 1:
            cols = pl.ds(h * HALF, HALF)
            remote(comb_send.at[u, j, :, cols], comb.at[u, y, :, cols], cbase[u] + y * 2 + h, (p, d, j))

    def comb_arrived(u, h):
        for w in others_y:
            arrived(comb.at[u, w, :, pl.ds(h * HALF, HALF)], cbase[u] + w * 2 + h)

    def combined(u, cols):
        v = own[:, cols]
        for w in others_y:
            v = v + comb[u, w, :, cols].astype(F32)
        return v

    relay(0)
    relay(1)
    send_own(2)
    r_b, sel_b, sg_b, sum_b = owner(0, K, 0)
    r_tok[...] = jnp.broadcast_to(r_b, r_tok.shape)
    finish(0)
    dispatch(0, K, rows_x, True)
    for c in weights:
        c.wait()
    project_up()
    finish(1)
    dispatch(1, K, rows_g, False)
    project_w()
    ones8 = jnp.ones((8, FFL), BF16)

    def activate(s, c):
        where = pl.ds(pl.multiple_of(s * CAP, CAP), CAP)
        r = r_row[where, 0:1]
        a, b, w = acc_a[where, :] * r, acc_b[where, :] * r, acc_w[where, :]
        sa = jax.nn.sigmoid(a)
        act = a * sa
        prod = (act * b).astype(BF16).astype(F32) * w
        hi, lo = split(prod)
        gs[s] = nt(ones8, hi) + nt(ones8, lo)
        grad[0, where, :] = (w * b * sa * (1.0 + a * (1.0 - sa))).astype(BF16)
        grad[1, where, :] = (w * act).astype(BF16)
        return c

    lax.fori_loop(0, ND, activate, 0)
    for o in range(ND):
        for v in range(NY):
            if o or v:
                s = lax.rem(d + o, ND)
                remote(gs.at[s], gr.at[d, y], gcbase + d * NY + y, (p, s, lax.rem(y + v, NY)))
    kept_gc = local(gs.at[d], gr.at[d, y])

    def back_rows(j, cols):
        return nt(grad[0], wgu[0, j, cols, :]) + nt(grad[1], wgu[1, j, cols, :])

    kept_b, kept_f = {}, {}
    for i in range(NY):
        for h in range(2):
            kept_b[i, h] = produce(0, i, h, back_rows)
        if i == 0:
            relay(2)
    owner(2, 0, 1)
    finish(2)
    dispatch(2, 0, rows_x, True)
    project_up()

    def act_forward(s, c):
        where = pl.ds(pl.multiple_of(s * CAP, CAP), CAP)
        r = r_row[where, 0:1]
        a, b = acc_a[where, :] * r, acc_b[where, :] * r
        inner[where, :] = (a * jax.nn.sigmoid(a) * b).astype(BF16)
        return c

    lax.fori_loop(0, ND, act_forward, 0)

    def forward_rows(j, cols):
        return nn(inner[...], wd[j, :, cols])

    for i in range(NY):
        for h in range(2):
            kept_f[i, h] = produce(1, i, h, forward_rows)
    for i in range(NY):
        for h in range(2):
            combine(0, i, h, kept_b[i, h])

    kept_gc.wait()
    for o in range(ND):
        for v in range(NY):
            if o or v:
                s, w = lax.rem(d + o, ND), lax.rem(y + v, NY)
                arrived(gr.at[s, w], gcbase + s * NY + w)
    gc = jnp.zeros((8, TOK), F32)
    for e in range(E):
        t = gr[e, 0]
        for v in range(1, NY):
            t = t + gr[e, v]
        gc = gc + jnp.where(row8 == e, nn(t.astype(BF16), hot[0, e]), 0.0)
    mixed = jnp.sum(gc * sg_b, axis=0, keepdims=True) / sum_b
    dl = jnp.where(sel_b > 0.5, ROUTE_SCALE * (gc - mixed) / sum_b * sg_b * (1.0 - sg_b), 0.0)
    dl_hi, dl_lo = split(jnp.transpose(jnp.concatenate([dl, jnp.zeros((TOK - 8, TOK), F32)], axis=0)))
    rpad[...] = jnp.zeros_like(rpad)
    rpad[0:8, :] = sm[y]
    for h in range(2):
        comb_arrived(0, h)

    def tail_one(n, tot):
        cols = pl.ds(pl.multiple_of(n * W, W), W)
        router = rpad[:, cols].astype(BF16)
        moe = combined(0, cols).astype(BF16).astype(F32)
        v = moe + nn(dl_hi, router) + nn(dl_lo, router)
        dm[:, cols] = v
        x = g_all[0, d, y, :, cols].astype(F32)
        gpart[d, :, cols] = jnp.sum(v * x * r_tok[:, 0:1], axis=0, keepdims=True)
        return tot + jnp.sum(v * sm[y, GAIN_ROW : GAIN_ROW + 1, cols] * x, axis=-1, keepdims=True)

    part = lax.fori_loop(0, tiles, tail_one, jnp.zeros((TOK, 1), F32))
    ip[y] = jnp.broadcast_to(part, (TOK, 128))
    for v in others_y:
        remote(ip.at[y], ip.at[y], ipbase + y, (p, d, v))
    for s in others_d:
        remote(gpart.at[d], gpart.at[d], gpbase + d, (p, s, y))
    for v in others_y:
        arrived(ip.at[v], ipbase + v)
    inner_sum = ip[0]
    for v in range(1, NY):
        inner_sum = inner_sum + ip[v]
    inner_sum = inner_sum[:, 0:1]

    def tail_two(n, c):
        cols = pl.ds(pl.multiple_of(n * W, W), W)
        r = r_tok[:, 0:1]
        h = dm[:, cols] * sm[y, GAIN_ROW : GAIN_ROW + 1, cols]
        x = g_all[0, d, y, :, cols].astype(F32)
        g = g_all[1, d, y, :, cols].astype(F32)
        ig[:, cols] = (g + r * h - x * (r * r * r) * inner_sum / D).astype(BF16)
        return c

    lax.fori_loop(0, tiles, tail_two, 0)

    def hand_on(src, dst, which, has, gets, where):
        i = counter["s"]
        counter["s"] += 1
        c = pltpu.make_async_remote_copy(
            src_ref=src, dst_ref=dst, send_sem=send_sem.at[i], recv_sem=recv_sem.at[zbase + which],
            device_id=where, device_id_type=MESH,
        )

        @pl.when(has)
        def _():
            c.start()

        @pl.when(jnp.logical_not(gets))
        def _():
            dst[...] = jnp.zeros_like(dst)

        def done():
            @pl.when(has)
            def _():
                c.wait_send()

            @pl.when(gets)
            def _():
                c.wait_recv()

        return done

    done_b = hand_on(ig, pb, 0, p > 0, p < NP - 1, (down, d, y))

    for i in range(NY - 1):
        for h in range(2):
            combine(1, i, h, kept_f[i, h])
    done_f = []
    for h in range(2):
        combine(1, NY - 1, h, kept_f[NY - 1, h])
        comb_arrived(1, h)

        def out_tile(n, c):
            cols = pl.ds(pl.multiple_of(h * HALF + n * BW, BW), BW)
            fo[:, cols] = (g_all[2, d, y, :, cols].astype(F32) + combined(1, cols)).astype(BF16)
            return c

        lax.fori_loop(0, HALF // BW, out_tile, 0)
        half = pl.ds(h * HALF, HALF)
        done_f.append(hand_on(fo.at[:, half], pf.at[:, half], 1 + h, p < NP - 1, p > 0, (up, d, y)))

    for s in others_d:
        arrived(gpart.at[s], gpbase + s)
    total = gpart[0]
    for s in range(1, ND):
        total = total + gpart[s]
    gg[...] = total
    for c in pending:
        c.wait_send()
    done_b()
    for done in done_f:
        done()


def local(mesh_sizes, entering, pending, stashed_in, forward_routes, backward_routes, norm_gains, w_router, w_gateup, w_down):
    NP, ND, NY = mesh_sizes
    _, TOK, DL = entering.shape
    K = forward_routes.shape[2]
    E = w_router.shape[2]
    FFL = w_gateup.shape[4]
    D = w_gateup.shape[2]
    CAP = TOK * K // E
    assert E == ND and E <= GAIN_ROW and 2 * K <= 8 and D == DL * NY
    wgu = jnp.transpose(w_gateup[0, 0], (1, 0, 2))
    cfg = (NP, ND, NY, TOK, DL, FFL, K, E, CAP)
    NS = E * CAP
    nsend = 3 * (2 * (ND // 2 + NY) * 4 + 4 * ND * NY) + 12 * ND * NY + 64
    nrecv = 3 * ND * NY * 2 + 5 * ND * NY + 4 * ND + 8 * NY + 16
    out = jax.ShapeDtypeStruct((TOK, DL), BF16)
    V = pltpu.VMEM
    res = pl.pallas_call(
        functools.partial(kernel, cfg),
        out_shape=[out, out, out, out, jax.ShapeDtypeStruct((1, DL), F32)],
        in_specs=[pl.BlockSpec(memory_space=pl.ANY)] * 5 + [pl.BlockSpec(memory_space=pltpu.VMEM)] * 4,
        out_specs=[pl.BlockSpec(memory_space=pltpu.VMEM)] * 5,
        scratch_shapes=[
            V((3, ND, NY, TOK, DL), BF16),
            V((ND, 8, TOK), jnp.int32),
            V((NY, 8, DL), F32),
            V((2, NY, DL, FFL), BF16),
            V((NY, FFL, DL), BF16),
            V((NY, NS, DL), BF16),
            V((NY, NS, DL), BF16),
            V((NS, FFL), F32),
            V((NS, FFL), F32),
            V((NS, FFL), F32),
            V((NS, FFL), BF16),
            V((2, NS, FFL), BF16),
            V((2, NY, ND, CAP, DL), BF16),
            V((2, NY, ND, CAP, DL), BF16),
            V((2, NY, TOK, DL), BF16),
            V((2, NY, TOK, DL), BF16),
            V((TOK, DL), F32),
            V((2, E, CAP, TOK), BF16),
            V((2, 2, TOK, NS), BF16),
            V((ND, 8, CAP), F32),
            V((ND, NY, 8, CAP), F32),
            V((TOK, DL), F32),
            V((NY, TOK, 128), F32),
            V((ND, 1, DL), F32),
            V((TOK, 128), F32),
            V((TOK, DL), F32),
            V((NS, 128), F32),
            pltpu.SemaphoreType.DMA((nsend,)),
            pltpu.SemaphoreType.DMA((nrecv,)),
            pltpu.SemaphoreType.DMA((64,)),
        ],
        compiler_params=pltpu.CompilerParams(
            collective_id=0, has_side_effects=True, vmem_limit_bytes=62 * 1024 * 1024
        ),
    )(
        stashed_in[0], pending[0], entering[0], wgu, w_down[0, 0],
        forward_routes[0].T, backward_routes[0].T, w_router[0].T, norm_gains,
    )
    fo, ig, pf, pb, gg = pl.pallas_call(
        settle,
        out_shape=[jax.ShapeDtypeStruct(v.shape, v.dtype) for v in res],
        in_specs=[pl.BlockSpec(memory_space=pl.ANY)] * 5,
        out_specs=[pl.BlockSpec(memory_space=pl.ANY)] * 5,
        scratch_shapes=[V(v.shape, v.dtype) for v in res] + [pltpu.SemaphoreType.DMA((10,))],
    )(*res)
    return fo[None], ig[None], pf[None], pb[None], gg


def solution(mesh):
    tokens = P("pipe", "dp", "expert")
    placed = (
        tokens, tokens, tokens,
        P("pipe", "dp", None), P("pipe", "dp", None),
        P("pipe", "expert"), P("pipe", "expert", None),
        P("pipe", "dp", None, None, "expert"), P("pipe", "dp", "expert", None),
    )
    sizes = tuple(mesh.shape[a] for a in ("pipe", "dp", "expert"))
    return jax.shard_map(
        functools.partial(local, sizes),
        mesh=mesh,
        in_specs=placed,
        out_specs=(tokens, tokens, tokens, tokens, P("pipe", "expert")),
        check_vma=False,
    )
```

```python
import functools

import jax
import jax.numpy as jnp
from jax import lax
from jax.experimental import pallas as pl
from jax.experimental.pallas import tpu as pltpu
from jax.sharding import PartitionSpec as P

ROUTE_SCALE = 2.827
EPSILON = 1e-05
F32 = jnp.float32
BF16 = jnp.bfloat16
MESH = pl.DeviceIdType.MESH
NT = (((1,), (1,)), ((), ()))
GAIN_ROW = 7


def nt(a, b):
    return lax.dot_general(a, b, NT, preferred_element_type=F32)


def nn(a, b):
    return jnp.dot(a, b, preferred_element_type=F32)


def split(v):
    hi = v.astype(BF16)
    return hi, (v - hi.astype(F32)).astype(BF16)


def settle(*refs):
    sources, targets, held, sem = refs[:5], refs[5:10], refs[10:15], refs[15]
    into = [pltpu.make_async_copy(a, b, sem.at[i]) for i, (a, b) in enumerate(zip(sources, held))]
    out = [pltpu.make_async_copy(a, b, sem.at[5 + i]) for i, (a, b) in enumerate(zip(held, targets))]
    for c in into:
        c.start()
    for a, b in zip(into, out):
        a.wait()
        b.start()
    for c in out:
        c.wait()


def lanes(v):
    total = v[:, 0:128]
    for i in range(1, v.shape[1] // 128):
        total = total + v[:, i * 128 : (i + 1) * 128]
    return total


def kernel(
    cfg,
    xb_in, gy_in, xf_in, wgu_in, wd_in, fr_in, br_in, router_in, gain_in,
    fo, ig, pf, pb, gg,
    g_all, rt, sm, wgu, wd, rows_x, rows_g, acc_a, acc_b, acc_w, inner, grad,
    ret_send, ret, comb_send, comb, own, hot, wts, gs, gr, dm, ip, gpart, r_tok, rpad, r_row,
    send_sem, recv_sem, local_sem,
):
    NP, ND, NY, TOK, DL, FFL, K, E, CAP = cfg
    HT = TOK // 2
    W = min(256, DL)
    tiles = DL // W
    BW = min(512, DL // 2)
    HALF = DL // 2
    NSLOT = E * CAP
    D = DL * NY
    p, d, y = lax.axis_index("pipe"), lax.axis_index("dp"), lax.axis_index("expert")
    core = lax.rem(d, 2)
    mate = d + 1 - 2 * core
    across = [lax.rem(d + 2 * o, ND) for o in range(1, ND // 2)]
    others_y = [lax.rem(y + o, NY) for o in range(1, NY)]
    others_d = [lax.rem(d + o, ND) for o in range(1, ND)]
    up, down = lax.rem(p + 1, NP), lax.rem(p + NP - 1, NP)

    counter = {"s": 0, "r": 0, "l": 0}
    pending = []

    def remote(src, dst, r_index, where):
        i = counter["s"]
        counter["s"] += 1
        c = pltpu.make_async_remote_copy(
            src_ref=src, dst_ref=dst, send_sem=send_sem.at[i], recv_sem=recv_sem.at[r_index],
            device_id=where, device_id_type=MESH,
        )
        c.start()
        pending.append(c)

    def arrived(ref, r_index):
        pltpu.make_async_remote_copy(
            src_ref=ref, dst_ref=ref, send_sem=send_sem.at[0], recv_sem=recv_sem.at[r_index],
            device_id=(p, d, y), device_id_type=MESH,
        ).wait_recv()

    def local(src, dst):
        i = counter["l"]
        counter["l"] += 1
        c = pltpu.make_async_copy(src, dst, local_sem.at[i])
        c.start()
        return c

    def block(n):
        base = counter["r"]
        counter["r"] += n
        return base

    first = [local(src, g_all.at[t, d, y]) for t, src in enumerate((xb_in, gy_in, xf_in))]
    rt[d] = jnp.full((8, TOK), -1, jnp.int32)
    rt[d, 0:K, :] = fr_in[...]
    rt[d, K : 2 * K, :] = br_in[...]
    sm[y] = jnp.zeros((8, DL), F32)
    sm[y, 0:E, :] = router_in[...].astype(F32)
    sm[y, GAIN_ROW : GAIN_ROW + 1, :] = gain_in[...]
    weights = [local(wgu_in.at[k, pl.ds(j * DL, DL)], wgu.at[k, j]) for k in range(2) for j in range(NY)]
    weights += [local(wd_in.at[:, pl.ds(j * DL, DL)], wd.at[j]) for j in range(NY)]

    barrier = pltpu.get_barrier_semaphore()
    for o in range(ND):
        for v in range(NY):
            if o or v:
                pl.semaphore_signal(
                    barrier, inc=1, device_id=(p, lax.rem(d + o, ND), lax.rem(y + v, NY)), device_id_type=MESH
                )
    pl.semaphore_signal(barrier, inc=1, device_id=(up, d, y), device_id_type=MESH)
    pl.semaphore_signal(barrier, inc=1, device_id=(down, d, y), device_id_type=MESH)
    pl.semaphore_wait(barrier, ND * NY + 1)
    for c in first:
        c.wait()

    gbase = block(3 * ND * NY * 2)

    def piece(t, dd, yy, h):
        return g_all.at[t, dd, yy, pl.ds(h * HT, HT)]

    def gsem(t, dd, yy, h):
        return gbase + ((t * ND + dd) * NY + yy) * 2 + h

    def gsend(t, dd, yy, h, where):
        ref = piece(t, dd, yy, h)
        remote(ref, ref, gsem(t, dd, yy, h), where)

    def gwait(t, dd, yy, h):
        arrived(piece(t, dd, yy, h), gsem(t, dd, yy, h))

    def send_own(t):
        for i in range(2):
            for x in across:
                gsend(t, d, y, i, (p, x, y))
            for v in others_y:
                gsend(t, d, y, 1 - i, (p, d, v))
        for i in range(2):
            gsend(t, d, y, i, (p, mate, y))

    def relay(t):
        for i in range(2):
            for x in across:
                gwait(t, x, y, i)
                if i == 0 or t == 2:
                    for v in others_y:
                        gsend(t, x, y, i, (p, d, v))
                gsend(t, x, y, i, (p, mate, y))
            for v in others_y:
                gwait(t, d, v, 1 - i)
                if i == 0 and t < 2:
                    for x in across:
                        gsend(t, d, v, 1, (p, x, y))
                gsend(t, d, v, 1 - i, (p, mate, y))

    def finish(t):
        for x in across:
            for v in others_y:
                for h in range(2):
                    gwait(t, x, v, h)
                    gsend(t, x, v, h, (p, mate, y))
        for dd in [mate] + [lax.rem(mate + 2 * o, ND) for o in range(1, ND // 2)]:
            for v in range(NY):
                for h in range(2):
                    gwait(t, dd, v, h)

    rbase, sbase = block(ND), block(NY)
    for s in others_d:
        remote(rt.at[d], rt.at[d], rbase + d, (p, s, y))
    for v in others_y:
        remote(sm.at[y], sm.at[y], sbase + y, (p, d, v))
    send_own(0)
    send_own(1)
    for s in others_d:
        arrived(rt.at[s], rbase + s)
    for v in others_y:
        arrived(sm.at[v], sbase + v)

    before = (
        lax.broadcasted_iota(jnp.int32, (TOK, TOK), 0) < lax.broadcasted_iota(jnp.int32, (TOK, TOK), 1)
    ).astype(F32).astype(BF16)
    row8 = lax.broadcasted_iota(jnp.int32, (8, TOK), 0)
    slot = lax.broadcasted_iota(jnp.int32, (CAP, TOK), 0).astype(F32)

    def one_hot(member_row, pos_row):
        return jnp.where(slot == pos_row, member_row, 0.0)

    def expert_hot(s, base):
        picks = rt[s]
        member = jnp.zeros((8, TOK), F32)
        for k in range(K):
            member += (picks[base + k : base + k + 1, :] == d).astype(F32)
        pos = nn(member.astype(BF16), before)
        return one_hot(member[0:1, :], pos[0:1, :]).astype(BF16)

    def dispatch(t, base, rows, scaled):
        PW = min(512, DL)

        def body(s, _):
            pick = expert_hot(s, base)
            where = pl.ds(pl.multiple_of(s * CAP, CAP), CAP)
            total = jnp.zeros((CAP, 128), F32)
            for j in range(NY):
                for i in range(DL // PW):
                    cols = pl.ds(i * PW, PW)
                    part = nn(pick, g_all[t, s, j, :, cols])
                    if scaled:
                        total = total + lanes(part * part)
                        part = part * sm[j, GAIN_ROW : GAIN_ROW + 1, cols]
                    rows[j, where, cols] = part.astype(BF16)
            if scaled:
                scaling = lax.rsqrt(jnp.sum(total, axis=-1, keepdims=True) / D + EPSILON)
                r_row[where, :] = jnp.broadcast_to(scaling, (CAP, 128))
            return 0

        lax.fori_loop(0, ND, body, 0)

    def project_up():
        acc_a[...] = jnp.zeros_like(acc_a)
        acc_b[...] = jnp.zeros_like(acc_b)
        KT = min(1024, DL)
        for j in range(NY):
            def body(i, c, j=j):
                ks = pl.ds(pl.multiple_of(i * KT, KT), KT)
                lhs = rows_x[j, :, ks]
                acc_a[...] += nn(lhs, wgu[0, j, ks, :])
                acc_b[...] += nn(lhs, wgu[1, j, ks, :])
                return c

            lax.fori_loop(0, DL // KT, body, 0)

    def project_w():
        acc_w[...] = jnp.zeros_like(acc_w)
        KT = min(1024, DL)
        for j in range(NY):
            def body(i, c, j=j):
                ks = pl.ds(pl.multiple_of(i * KT, KT), KT)
                acc_w[...] += nt(rows_g[j, :, ks], wd[j, :, ks])
                return c

            lax.fori_loop(0, DL // KT, body, 0)

    def owner(t, base, u):
        def squares(j, tot):
            def step(i, tt):
                v = g_all[t, d, j, :, pl.ds(pl.multiple_of(i * W, W), W)].astype(F32)
                return tt + lanes(v * v)

            return lax.fori_loop(0, tiles, step, tot, unroll=2)

        total = lax.fori_loop(0, NY, squares, jnp.zeros((TOK, 128), F32))
        total = jnp.sum(total, axis=-1, keepdims=True)
        scaling = lax.rsqrt(total / D + EPSILON)

        def logit(j, acc):
            def step(i, a):
                cols = pl.ds(pl.multiple_of(i * W, W), W)
                v = g_all[t, d, j, :, cols].astype(F32) * scaling * sm[j, GAIN_ROW : GAIN_ROW + 1, cols]
                return a + nt(sm[j, :, cols].astype(BF16), v.astype(BF16))

            return lax.fori_loop(0, tiles, step, acc, unroll=2)

        logits = lax.fori_loop(0, NY, logit, jnp.zeros((8, TOK), F32))
        picks = rt[d]
        sel = jnp.zeros((8, TOK), F32)
        for k in range(K):
            sel += (picks[base + k : base + k + 1, :] == row8).astype(F32)
        pos = nn(sel.astype(BF16), before)
        sg = jnp.where(sel > 0.5, jax.nn.sigmoid(logits), 0.0)
        total_sg = jnp.sum(sg, axis=0, keepdims=True)
        gate = ROUTE_SCALE * sg / total_sg
        weighted = []
        for e in range(E):
            h = one_hot(sel[e : e + 1, :], pos[e : e + 1, :])
            hot[u, e] = h.astype(BF16)
            weighted.append(h * gate[e : e + 1, :])
        g = jnp.transpose(jnp.concatenate(weighted, axis=0))
        hi, lo = split(g)
        wts[u, 0] = hi
        wts[u, 1] = lo
        return scaling, sel, sg, total_sg

    retbase = [block(NY * ND * 2) for _ in range(2)]
    cbase = [block(2 * NY) for _ in range(2)]
    gcbase, ipbase, gpbase, zbase = block(ND * NY), block(NY), block(ND), block(3)

    def chunk_of(i):
        return lax.rem(y + 1 + i, NY)

    def back(ref, u, j, s, h):
        return ref.at[u, j, s, :, pl.ds(h * HALF, HALF)]

    def produce(u, i, h, make):
        j = chunk_of(i)

        def body(n, c):
            cols = pl.ds(pl.multiple_of(h * HALF + n * BW, BW), BW)
            ret_send[u, j, :, :, cols] = make(j, cols).astype(BF16).reshape(ND, CAP, BW)
            return c

        lax.fori_loop(0, HALF // BW, body, 0, unroll=True)
        for s in others_d:
            remote(back(ret_send, u, j, s, h), back(ret, u, j, d, h), retbase[u] + (j * ND + d) * 2 + h, (p, s, y))
        return local(back(ret_send, u, j, d, h), back(ret, u, j, d, h))

    def combine(u, i, h, kept):
        j = chunk_of(i)
        for s in others_d:
            arrived(back(ret, u, j, s, h), retbase[u] + (j * ND + s) * 2 + h)
        kept.wait()

        def body(n, c):
            cols = pl.ds(pl.multiple_of(h * HALF + n * BW, BW), BW)
            r = ret[u, j, :, :, cols].reshape(NSLOT, BW)
            v = nn(wts[u, 0], r) + nn(wts[u, 1], r)
            if i < NY - 1:
                comb_send[u, j, :, cols] = v.astype(BF16)
            else:
                own[:, cols] = v
            return c

        lax.fori_loop(0, HALF // BW, body, 0, unroll=True)
        if i < NY - 1:
            cols = pl.ds(h * HALF, HALF)
            remote(comb_send.at[u, j, :, cols], comb.at[u, y, :, cols], cbase[u] + y * 2 + h, (p, d, j))

    def comb_arrived(u, h):
        for w in others_y:
            arrived(comb.at[u, w, :, pl.ds(h * HALF, HALF)], cbase[u] + w * 2 + h)

    def combined(u, cols):
        v = own[:, cols]
        for w in others_y:
            v = v + comb[u, w, :, cols].astype(F32)
        return v

    relay(0)
    relay(1)
    send_own(2)
    r_b, sel_b, sg_b, sum_b = owner(0, K, 0)
    r_tok[...] = jnp.broadcast_to(r_b, r_tok.shape)
    finish(0)
    dispatch(0, K, rows_x, True)
    for c in weights:
        c.wait()
    project_up()
    finish(1)
    dispatch(1, K, rows_g, False)
    project_w()
    ones8 = jnp.ones((8, FFL), BF16)

    def activate(s, c):
        where = pl.ds(pl.multiple_of(s * CAP, CAP), CAP)
        r = r_row[where, 0:1]
        a, b, w = acc_a[where, :] * r, acc_b[where, :] * r, acc_w[where, :]
        sa = jax.nn.sigmoid(a)
        act = a * sa
        prod = (act * b).astype(BF16).astype(F32) * w
        hi, lo = split(prod)
        gs[s] = nt(ones8, hi) + nt(ones8, lo)
        grad[0, where, :] = (w * b * sa * (1.0 + a * (1.0 - sa))).astype(BF16)
        grad[1, where, :] = (w * act).astype(BF16)
        return c

    lax.fori_loop(0, ND, activate, 0)
    for o in range(ND):
        for v in range(NY):
            if o or v:
                s = lax.rem(d + o, ND)
                remote(gs.at[s], gr.at[d, y], gcbase + d * NY + y, (p, s, lax.rem(y + v, NY)))
    kept_gc = local(gs.at[d], gr.at[d, y])

    def back_rows(j, cols):
        return nt(grad[0], wgu[0, j, cols, :]) + nt(grad[1], wgu[1, j, cols, :])

    kept_b, kept_f = {}, {}
    for i in range(NY):
        for h in range(2):
            kept_b[i, h] = produce(0, i, h, back_rows)
        if i == 0:
            relay(2)
    owner(2, 0, 1)
    finish(2)
    dispatch(2, 0, rows_x, True)
    project_up()

    def act_forward(s, c):
        where = pl.ds(pl.multiple_of(s * CAP, CAP), CAP)
        r = r_row[where, 0:1]
        a, b = acc_a[where, :] * r, acc_b[where, :] * r
        inner[where, :] = (a * jax.nn.sigmoid(a) * b).astype(BF16)
        return c

    lax.fori_loop(0, ND, act_forward, 0)

    def forward_rows(j, cols):
        return nn(inner[...], wd[j, :, cols])

    for i in range(NY):
        for h in range(2):
            kept_f[i, h] = produce(1, i, h, forward_rows)
    for i in range(NY):
        for h in range(2):
            combine(0, i, h, kept_b[i, h])

    kept_gc.wait()
    for o in range(ND):
        for v in range(NY):
            if o or v:
                s, w = lax.rem(d + o, ND), lax.rem(y + v, NY)
                arrived(gr.at[s, w], gcbase + s * NY + w)
    gc = jnp.zeros((8, TOK), F32)
    for e in range(E):
        t = gr[e, 0]
        for v in range(1, NY):
            t = t + gr[e, v]
        gc = gc + jnp.where(row8 == e, nn(t.astype(BF16), hot[0, e]), 0.0)
    mixed = jnp.sum(gc * sg_b, axis=0, keepdims=True) / sum_b
    dl = jnp.where(sel_b > 0.5, ROUTE_SCALE * (gc - mixed) / sum_b * sg_b * (1.0 - sg_b), 0.0)
    dl_hi, dl_lo = split(jnp.transpose(jnp.concatenate([dl, jnp.zeros((TOK - 8, TOK), F32)], axis=0)))
    rpad[...] = jnp.zeros_like(rpad)
    rpad[0:8, :] = sm[y]
    for h in range(2):
        comb_arrived(0, h)

    def tail_one(n, tot):
        cols = pl.ds(pl.multiple_of(n * W, W), W)
        router = rpad[:, cols].astype(BF16)
        moe = combined(0, cols).astype(BF16).astype(F32)
        v = moe + nn(dl_hi, router) + nn(dl_lo, router)
        dm[:, cols] = v
        x = g_all[0, d, y, :, cols].astype(F32)
        gpart[d, :, cols] = jnp.sum(v * x * r_tok[:, 0:1], axis=0, keepdims=True)
        return tot + jnp.sum(v * sm[y, GAIN_ROW : GAIN_ROW + 1, cols] * x, axis=-1, keepdims=True)

    part = lax.fori_loop(0, tiles, tail_one, jnp.zeros((TOK, 1), F32))
    ip[y] = jnp.broadcast_to(part, (TOK, 128))
    for v in others_y:
        remote(ip.at[y], ip.at[y], ipbase + y, (p, d, v))
    for s in others_d:
        remote(gpart.at[d], gpart.at[d], gpbase + d, (p, s, y))
    for v in others_y:
        arrived(ip.at[v], ipbase + v)
    inner_sum = ip[0]
    for v in range(1, NY):
        inner_sum = inner_sum + ip[v]
    inner_sum = inner_sum[:, 0:1]

    def tail_two(n, c):
        cols = pl.ds(pl.multiple_of(n * W, W), W)
        r = r_tok[:, 0:1]
        h = dm[:, cols] * sm[y, GAIN_ROW : GAIN_ROW + 1, cols]
        x = g_all[0, d, y, :, cols].astype(F32)
        g = g_all[1, d, y, :, cols].astype(F32)
        ig[:, cols] = (g + r * h - x * (r * r * r) * inner_sum / D).astype(BF16)
        return c

    lax.fori_loop(0, tiles, tail_two, 0)

    def hand_on(src, dst, which, has, gets, where):
        i = counter["s"]
        counter["s"] += 1
        c = pltpu.make_async_remote_copy(
            src_ref=src, dst_ref=dst, send_sem=send_sem.at[i], recv_sem=recv_sem.at[zbase + which],
            device_id=where, device_id_type=MESH,
        )

        @pl.when(has)
        def _():
            c.start()

        @pl.when(jnp.logical_not(gets))
        def _():
            dst[...] = jnp.zeros_like(dst)

        def done():
            @pl.when(has)
            def _():
                c.wait_send()

            @pl.when(gets)
            def _():
                c.wait_recv()

        return done

    done_b = hand_on(ig, pb, 0, p > 0, p < NP - 1, (down, d, y))

    for i in range(NY - 1):
        for h in range(2):
            combine(1, i, h, kept_f[i, h])
    done_f = []
    for h in range(2):
        combine(1, NY - 1, h, kept_f[NY - 1, h])
        comb_arrived(1, h)

        def out_tile(n, c):
            cols = pl.ds(pl.multiple_of(h * HALF + n * BW, BW), BW)
            fo[:, cols] = (g_all[2, d, y, :, cols].astype(F32) + combined(1, cols)).astype(BF16)
            return c

        lax.fori_loop(0, HALF // BW, out_tile, 0)
        half = pl.ds(h * HALF, HALF)
        done_f.append(hand_on(fo.at[:, half], pf.at[:, half], 1 + h, p < NP - 1, p > 0, (up, d, y)))

    for s in others_d:
        arrived(gpart.at[s], gpbase + s)
    total = gpart[0]
    for s in range(1, ND):
        total = total + gpart[s]
    gg[...] = total
    for c in pending:
        c.wait_send()
    done_b()
    for done in done_f:
        done()


def local(mesh_sizes, entering, pending, stashed_in, forward_routes, backward_routes, norm_gains, w_router, w_gateup, w_down):
    NP, ND, NY = mesh_sizes
    _, TOK, DL = entering.shape
    K = forward_routes.shape[2]
    E = w_router.shape[2]
    FFL = w_gateup.shape[4]
    D = w_gateup.shape[2]
    CAP = TOK * K // E
    assert E == ND and E <= GAIN_ROW and 2 * K <= 8 and D == DL * NY
    wgu = jnp.transpose(w_gateup[0, 0], (1, 0, 2))
    cfg = (NP, ND, NY, TOK, DL, FFL, K, E, CAP)
    NS = E * CAP
    nsend = 3 * (2 * (ND // 2 + NY) * 4 + 4 * ND * NY) + 12 * ND * NY + 64
    nrecv = 3 * ND * NY * 2 + 5 * ND * NY + 4 * ND + 8 * NY + 16
    out = jax.ShapeDtypeStruct((TOK, DL), BF16)
    V = pltpu.VMEM
    res = pl.pallas_call(
        functools.partial(kernel, cfg),
        out_shape=[out, out, out, out, jax.ShapeDtypeStruct((1, DL), F32)],
        in_specs=[pl.BlockSpec(memory_space=pl.ANY)] * 5 + [pl.BlockSpec(memory_space=pltpu.VMEM)] * 4,
        out_specs=[pl.BlockSpec(memory_space=pltpu.VMEM)] * 5,
        scratch_shapes=[
            V((3, ND, NY, TOK, DL), BF16),
            V((ND, 8, TOK), jnp.int32),
            V((NY, 8, DL), F32),
            V((2, NY, DL, FFL), BF16),
            V((NY, FFL, DL), BF16),
            V((NY, NS, DL), BF16),
            V((NY, NS, DL), BF16),
            V((NS, FFL), F32),
            V((NS, FFL), F32),
            V((NS, FFL), F32),
            V((NS, FFL), BF16),
            V((2, NS, FFL), BF16),
            V((2, NY, ND, CAP, DL), BF16),
            V((2, NY, ND, CAP, DL), BF16),
            V((2, NY, TOK, DL), BF16),
            V((2, NY, TOK, DL), BF16),
            V((TOK, DL), F32),
            V((2, E, CAP, TOK), BF16),
            V((2, 2, TOK, NS), BF16),
            V((ND, 8, CAP), F32),
            V((ND, NY, 8, CAP), F32),
            V((TOK, DL), F32),
            V((NY, TOK, 128), F32),
            V((ND, 1, DL), F32),
            V((TOK, 128), F32),
            V((TOK, DL), F32),
            V((NS, 128), F32),
            pltpu.SemaphoreType.DMA((nsend,)),
            pltpu.SemaphoreType.DMA((nrecv,)),
            pltpu.SemaphoreType.DMA((64,)),
        ],
        compiler_params=pltpu.CompilerParams(
            collective_id=0, has_side_effects=True, vmem_limit_bytes=62 * 1024 * 1024
        ),
    )(
        stashed_in[0], pending[0], entering[0], wgu, w_down[0, 0],
        forward_routes[0].T, backward_routes[0].T, w_router[0].T, norm_gains,
    )
    fo, ig, pf, pb, gg = pl.pallas_call(
        settle,
        out_shape=[jax.ShapeDtypeStruct(v.shape, v.dtype) for v in res],
        in_specs=[pl.BlockSpec(memory_space=pl.ANY)] * 5,
        out_specs=[pl.BlockSpec(memory_space=pl.ANY)] * 5,
        scratch_shapes=[V(v.shape, v.dtype) for v in res] + [pltpu.SemaphoreType.DMA((10,))],
    )(*res)
    return fo[None], ig[None], pf[None], pb[None], gg


def solution(mesh):
    tokens = P("pipe", "dp", "expert")
    placed = (
        tokens, tokens, tokens,
        P("pipe", "dp", None), P("pipe", "dp", None),
        P("pipe", "expert"), P("pipe", "expert", None),
        P("pipe", "dp", None, None, "expert"), P("pipe", "dp", "expert", None),
    )
    sizes = tuple(mesh.shape[a] for a in ("pipe", "dp", "expert"))
    return jax.shard_map(
        functools.partial(local, sizes),
        mesh=mesh,
        in_specs=placed,
        out_specs=(tokens, tokens, tokens, tokens, P("pipe", "expert")),
        check_vma=False,
    )
```
